32 devices in a mesh: fsdp: 4 (over y, x), tensor: 8 (over z, core).
Axes of the slice: x: 2, y: 2, z: 4, core: 2. Of those that a mesh axis runs over, the one named last changes fastest.
Arguments:
- modality: int32 [4096], P('fsdp'), may hold values from 0 to 2, as said below
- out_grad: bfloat16 [4096, 4096], P('fsdp', 'tensor'), may hold values from -6 to 6
- gate_pre: bfloat16 [4096, 11008], P('fsdp', 'tensor'), may hold values from -6 to 6
- up_pre: bfloat16 [4096, 11008], P('fsdp', 'tensor'), may hold values from -6 to 6
- down_weight: bfloat16 [3, 11008, 4096], P(None, 'tensor', 'fsdp'), may hold values from -0.0546875 to 0.0546875
Outputs:
- down_grad: float32 [3, 11008, 4096], P(None, 'tensor', 'fsdp')
- gate_grad: bfloat16 [4096, 11008], P('fsdp', 'tensor')
- up_grad: bfloat16 [4096, 11008], P('fsdp', 'tensor')
The draws below stay inside these ranges and needn't reach their ends.
Inputs may be any that keep to these rules, and one draw needn't show every extreme that they name: `modality`: the 1024 tokens of every index of fsdp hold each of the three modalities at least once.
All inputs are finite; a program needn't handle non-finite values.
Results may differ from the reference program's by a relative error of at most 0.012.
Values may be sent and summed in bfloat16 or wider, within the bound.
A program may use at most 256 MiB of HBM per device.

```python
import jax
import jax.numpy as jnp
from jax import lax

D = 4096
FF = 11008
TOK_DEV = 1024
TOKENS = 4096
N_FSDP = 4


def draw_modality(key, part):
    subkeys = jax.random.split(jax.random.fold_in(key, 11), 4)
    groups = TOKENS // TOK_DEV
    position = jnp.arange(TOKENS, dtype=jnp.int32)
    group_id = position // TOK_DEV
    local_pos = position % TOK_DEV
    rotation = jax.random.randint(subkeys[0], (), 0, 3)
    leader = (jnp.arange(groups, dtype=jnp.int32) + rotation) % 3
    shares = jax.random.randint(subkeys[1], (groups,), 3, 9)
    offsets = jax.random.randint(subkeys[2], (groups,), 0, TOK_DEV)
    rolls = jax.random.randint(subkeys[3], (TOKENS,), 0, 20)
    lead_kind = leader[group_id]
    base_kind = jnp.where(rolls < 2 * shares[group_id], lead_kind, (lead_kind + 1 + rolls % 2) % 3)
    distance = (local_pos - offsets[group_id]) % TOK_DEV
    return jnp.where(distance < 3, distance, base_kind).astype(jnp.int32)


def spiked(entries, stream_key, source, target, shards_of, factor):
    owner, partner = [(jnp.arange(entries.shape[axis_at]) // (entries.shape[axis_at] // shards_of)).reshape([-1 if axis == axis_at else 1 for axis in range(entries.ndim)]) for axis_at in (source, target)]
    chosen = jax.random.permutation(stream_key, shards_of)[partner]
    strong = (owner == chosen) | (owner == (partner + shards_of // 2) % shards_of)
    return jnp.where(strong, factor * entries, entries)


def block_scale(rng, shape, pieces, smallest, high):
    def one(dim, shards_of):
        heights = jax.random.uniform(jax.random.fold_in(jax.random.fold_in(rng, 6), dim), (shards_of,), jnp.float32, smallest / len(pieces), high / len(pieces))
        return jnp.repeat(jnp.exp(heights), shape[dim] // shards_of).reshape((-1,) + (1,) * (len(shape) - dim - 1))

    factor_of = one(*pieces[0])
    for cut in pieces[1:]:
        factor_of = factor_of * one(*cut)
    return factor_of


def gaussian(stream_key, shape, deviation, bound, cuts=(), kind=jnp.bfloat16):
    loudness = block_scale(stream_key, shape, cuts, -0.22, 0.18) if cuts else 1.0
    drawn = jax.random.normal(stream_key, shape, jnp.float32) * deviation * loudness
    return jnp.minimum(jnp.maximum(drawn, -bound), bound).astype(kind)


def gaussian_with(own_key, dims, width, bound, cuts, heavy, kind=jnp.bfloat16):
    array = width * jax.random.normal(own_key, dims, jnp.float32)
    if cuts:
        array = array * block_scale(own_key, dims, cuts, -0.22, 0.18)
    return jnp.clip(spiked(array, jax.random.fold_in(own_key, 3), *heavy), -bound, bound).astype(kind)


def setup_inputs(seed: int = 0) -> dict:
    keys = jax.random.split(jax.random.key(seed), 6)
    modality = draw_modality(jax.random.fold_in(keys[5], 71), 0)
    out_grad = gaussian_with(keys[1], (TOKENS, D), 1.0, 6.0, ((0, 4), (1, 8)), (0, 1, 8, 2.0))
    gate_pre = gaussian(keys[2], (TOKENS, FF), 1.0, 6.0, ((0, 4), (1, 8)))
    up_pre = gaussian(keys[3], (TOKENS, FF), 1.0, 6.0, ((0, 4), (1, 8)))
    down_weight = gaussian(keys[4], (3, FF, D), FF ** -0.5, 0.0546875, ((1, 8), (2, 4)))
    return dict(modality=modality, out_grad=out_grad, gate_pre=gate_pre, up_pre=up_pre, down_weight=down_weight)


def reference(modality, out_grad, gate_pre, up_pre, down_weight):
    labels = jnp.arange(3, dtype=jnp.int32)
    kind_onehot = (modality[:, None] == labels[None, :]).astype(jnp.float32)
    counts = jnp.sum(kind_onehot, axis=0)
    factor = TOKENS / (3.0 * counts)
    token_scale = jnp.sum(kind_onehot * factor[None, :], axis=1)
    scaled = (out_grad.astype(jnp.float32) * token_scale[:, None]).astype(jnp.bfloat16)
    gate_val = gate_pre.astype(jnp.float32)
    up_val = up_pre.astype(jnp.float32)
    sigmoid_g = jax.nn.sigmoid(gate_val)
    active = gate_val * sigmoid_g
    hidden = (active * up_val).astype(jnp.bfloat16)
    kind_marks = kind_onehot.T.astype(jnp.bfloat16)
    d_hidden = jnp.zeros((TOKENS, FF), jnp.float32)
    for kind_id in range(3):
        masked = scaled * kind_marks[kind_id][:, None]
        d_hidden = d_hidden + lax.dot_general(masked, down_weight[kind_id], (((1,), (1,)), ((), ())), preferred_element_type=jnp.float32)
    up_grad = (d_hidden * active).astype(jnp.bfloat16)
    slope = sigmoid_g * (1.0 + gate_val * (1.0 - sigmoid_g))
    gate_grad = (d_hidden * up_val * slope).astype(jnp.bfloat16)
    group_hidden = hidden.reshape(N_FSDP, TOK_DEV, FF)
    group_scaled = scaled.reshape(N_FSDP, TOK_DEV, D)
    group_marks = jnp.transpose(kind_marks.reshape(3, N_FSDP, TOK_DEV), (1, 0, 2))

    def one_group(running, group_items):
        rows_hidden, rows_scaled, marks_here = group_items
        partials = []
        for kind_id in range(3):
            masked = rows_scaled * marks_here[kind_id][:, None]
            product = lax.dot_general(rows_hidden, masked, (((0,), (0,)), ((), ())), preferred_element_type=jnp.float32)
            partials.append(lax.optimization_barrier(product.astype(jnp.bfloat16)).astype(jnp.float32))
        return running + jnp.stack(partials), None

    down_grad, _ = lax.scan(one_group, jnp.zeros((3, FF, D), jnp.float32), (group_hidden, group_scaled, group_marks))
    return down_grad, gate_grad, up_grad
```

```python
import jax
import jax.numpy as jnp
from jax import lax
from jax.sharding import PartitionSpec as P


def kind_table(kind_ids):
    labels = jnp.arange(3, dtype=jnp.int32)
    return (kind_ids[:, None] == labels[None, :]).astype(jnp.float32)


def swap(values, axis, size, step):
    return lax.ppermute(values, axis, [(i, i ^ step) for i in range(size)])


def shards(modality, out_grad, gate_pre, up_pre, down_weight):
    rows, block = out_grad.shape
    groups = lax.axis_size("fsdp")
    lanes = lax.axis_size("tensor")
    width = down_weight.shape[2]
    half = rows // 2
    me = lax.axis_index("fsdp")
    core = lax.axis_index("tensor") % 2
    pieces = width // (2 * block)

    cores = [[i for i in range(lanes) if i % 2 == c] for c in range(2)]
    stripe = lax.all_gather(out_grad, "tensor", axis=0, axis_index_groups=cores)
    stripe = stripe.reshape(groups, pieces, rows, block)

    gate_val = gate_pre.astype(jnp.float32)
    up_val = up_pre.astype(jnp.float32)
    sigmoid_g = jax.nn.sigmoid(gate_val)
    active = gate_val * sigmoid_g
    hidden = (active * up_val).astype(jnp.bfloat16)
    if groups == 4:
        hid1 = swap(hidden, "fsdp", groups, 1)
        hid2 = swap(hidden, "fsdp", groups, 2)
        hid3a = swap(hid2[:half], "fsdp", groups, 1)
        hid3b = swap(hid1[half:], "fsdp", groups, 2)
        hid_list = [hidden, hid1, hid2, hid3a, hid3b]
    else:
        hid_list = [hidden] + [swap(hidden, "fsdp", groups, k) for k in range(1, groups)]

    kinds = lax.all_gather(modality, "fsdp", axis=0)
    counts = jnp.sum(kind_table(kinds.reshape(-1)), axis=0)
    factor = rows * groups / (3.0 * counts)

    order = [groups - 1] + list(range(1, groups - 1)) + [0]
    onehots, scaled = {}, {}
    for k in order:
        part = lax.dynamic_index_in_dim(stripe, me ^ k, 0, keepdims=False)
        if k:
            part = swap(part, "fsdp", groups, k)
        other = swap(part, "tensor", lanes, 1)
        first = jnp.where(core == 0, part, other)
        second = jnp.where(core == 0, other, part)
        joined = jnp.stack([first, second], axis=1).reshape(2 * pieces, rows, block)
        joined = jnp.concatenate([joined[i] for i in range(2 * pieces)], axis=1)
        onehots[k] = kind_table(lax.dynamic_index_in_dim(kinds, me ^ k, 0, keepdims=False))
        token_scale = jnp.sum(onehots[k] * factor[None, :], axis=1)
        scaled[k] = (joined.astype(jnp.float32) * token_scale[:, None]).astype(jnp.bfloat16)

    def back(k, lo, hi):
        marks = onehots[k][lo:hi].T.astype(jnp.bfloat16)
        masked = scaled[k][None, lo:hi, :] * marks[:, :, None]
        return lax.dot_general(
            masked, down_weight, (((0, 2), (0, 2)), ((), ())), preferred_element_type=jnp.float32
        )

    if groups == 4:
        far = back(3, 0, rows).astype(jnp.bfloat16)
        via1 = swap(far[:half], "fsdp", groups, 1)
        via2 = swap(far[half:], "fsdp", groups, 2)
        got2b = swap(back(2, half, rows).astype(jnp.bfloat16), "fsdp", groups, 2)
        got1a = swap(back(1, 0, half).astype(jnp.bfloat16), "fsdp", groups, 1)
        near2 = (back(2, 0, half) + via1.astype(jnp.float32)).astype(jnp.bfloat16)
        near1 = (back(1, half, rows) + via2.astype(jnp.float32)).astype(jnp.bfloat16)
        got2a = swap(near2, "fsdp", groups, 2)
        got1b = swap(near1, "fsdp", groups, 1)
        got1 = jnp.concatenate([got1a, got1b], axis=0).astype(jnp.float32)
        got2 = jnp.concatenate([got2a, got2b], axis=0).astype(jnp.float32)
        folded = back(0, 0, rows) + got1 + got2
    else:
        folded = back(0, 0, rows)
        for k in range(1, groups):
            got = swap(back(k, 0, rows).astype(jnp.bfloat16), "fsdp", groups, k)
            folded = folded + got.astype(jnp.float32)

    up_grad = (folded * active).astype(jnp.bfloat16)
    slope = sigmoid_g * (1.0 + gate_val * (1.0 - sigmoid_g))
    gate_grad = (folded * up_val * slope).astype(jnp.bfloat16)

    near_order = list(range(groups))
    hid_all = jnp.concatenate(hid_list, axis=0)
    scaled_all = jnp.concatenate([scaled[k] for k in near_order], axis=0)
    marks_all = jnp.concatenate([onehots[k] for k in near_order], axis=0).T.astype(jnp.bfloat16)
    masked_all = scaled_all[None, :, :] * marks_all[:, :, None]
    stacked = jnp.broadcast_to(hid_all[None, :, :], (3,) + hid_all.shape)
    down_grad = lax.dot_general(
        stacked, masked_all, (((1,), (1,)), ((0,), (0,))), preferred_element_type=jnp.float32
    )
    return (down_grad, gate_grad, up_grad)


def solution(mesh):
    placed = (
        P("fsdp"),
        P("fsdp", "tensor"),
        P("fsdp", "tensor"),
        P("fsdp", "tensor"),
        P(None, "tensor", "fsdp"),
    )
    return jax.shard_map(
        shards,
        mesh=mesh,
        in_specs=placed,
        out_specs=(P(None, "tensor", "fsdp"), P("fsdp", "tensor"), P("fsdp", "tensor")),
        check_vma=False,
    )
```
